32 devices in a mesh: gy: 8 (over z, x), gx: 4 (over y, core).
Axes of the slice: x: 2, y: 2, z: 4, core: 2. Of those that a mesh axis runs over, the one named last changes fastest.
Arguments:
- right_side: float32 [32, 512, 512], P(None, 'gy', 'gx'), may hold values from -32 to 32
- couplings: float32 [3, 512, 512], P(None, 'gy', 'gx'), may hold values from 0.1 to 0.5
- center: float32 [512, 512], P('gy', 'gx'), may hold values from 0.6 to 1.5
- ocean_mask: int32 [512, 512], P('gy', 'gx'), may hold values 0 or 1
Outputs:
- solution: float32 [32, 512, 512], P(None, 'gy', 'gx')
- residual: float32 [32, 512, 512], P(None, 'gy', 'gx')
The draws below stay inside these ranges and needn't reach their ends.
All inputs are finite; a program needn't handle non-finite values. No bound on the sum of `ocean_mask` on one device may be relied on, other than what follows from the above.
Results may differ from the reference program's by a relative error of at most 0.0055.
Values sent between devices are 32-bit elements; how exact they have to be, the bound alone decides.
A program may use at most 64 MiB of HBM per device.

```python
import math
import jax
import jax.numpy as jnp
from jax import lax

MEMBERS = 32
ITERS = 6
NLAT = 512
NLON = 512


def draw_right_side(key, part):
    key_base = jax.random.fold_in(key, 0)
    latitude = jnp.arange(NLAT, dtype=jnp.float32) / max(NLAT - 1, 1)
    rising = (1.0 + 2.0 * latitude)[None, :, None]
    base = jnp.clip(jax.random.normal(key_base, (MEMBERS, NLAT, NLON), jnp.float32), -5.0, 5.0)
    return base * rising


def place_ends(array, stream_key, least, top_value):
    longest = array.shape.index(max(array.shape))
    spots = []
    for shift in (0, 1):
        where = [jax.random.randint(jax.random.fold_in(stream_key, axis), (), 0, length) for axis, length in enumerate(array.shape)]
        where[longest] = (where[longest] + shift) % array.shape[longest]
        spots.append(tuple(where))
    return array.at[spots[0]].set(least).at[spots[1]].set(top_value)


def block_levels(key, extent, cuts, least, top_value):
    level = 1.0
    for dim, parts in cuts:
        steps = jax.random.uniform(jax.random.fold_in(jax.random.fold_in(key, 6), dim), (parts,), jnp.float32, least / len(cuts), top_value / len(cuts))
        level = level * jnp.repeat(jnp.exp(steps), extent[dim] // parts).reshape((-1,) + (1,) * (len(extent) - 1 - dim))
    return level


def setup_inputs(seed: int = 0) -> dict:
    keys = jax.random.split(jax.random.key(seed), 5)
    return {
        "right_side": draw_right_side(jax.random.fold_in(keys[4], 71), 0),
        "couplings": jnp.clip(jnp.exp(math.log(0.5) - 1.609438 * jax.random.uniform(keys[1], (3, NLAT, NLON), jnp.float32) ** block_levels(keys[1], (3, NLAT, NLON), ((1, 8), (2, 4)), -0.2, 0.2)), 0.1, 0.5),
        "center": jnp.clip(jnp.exp(math.log(1.5) - 0.9162907 * jax.random.uniform(keys[2], (NLAT, NLON), jnp.float32) ** block_levels(keys[2], (NLAT, NLON), ((0, 8), (1, 4)), -0.2, 0.2)), 0.6, 1.5),
        "ocean_mask": place_ends((jax.random.randint(keys[3], (NLAT, NLON), 0, 10) < 9).astype(jnp.int32), jax.random.fold_in(keys[3], 1), 0, 1),
    }


def extend_field(field):
    north_row = field[-1, ::-1]
    lat_padded = jnp.concatenate([jnp.zeros((1, field.shape[1]), jnp.float32), field, north_row[None, :]], axis=0)
    return jnp.concatenate([lat_padded[:, -1:], lat_padded, lat_padded[:, :1]], axis=1)


def coupling_terms(couplings):
    north_c = couplings[0]
    east_c = couplings[1]
    corner_c = couplings[2]
    zero_row = jnp.zeros((1, north_c.shape[1]), jnp.float32)
    north_s = jnp.concatenate([zero_row, north_c[:-1]], axis=0)
    east_w = jnp.roll(east_c, 1, axis=1)
    corner_s = jnp.concatenate([zero_row, corner_c[:-1]], axis=0)
    corner_w = jnp.roll(corner_c, 1, axis=1)
    corner_sw = jnp.roll(corner_s, 1, axis=1)
    return (north_c, north_s, east_c, east_w, corner_c, corner_s, corner_w, corner_sw)


def operate(field, terms, diag_total, oceanf):
    padded = extend_field(field)
    beside = terms[0] * padded[2:, 1:-1] + terms[1] * padded[:-2, 1:-1]
    beside = beside + terms[2] * padded[1:-1, 2:] + terms[3] * padded[1:-1, :-2]
    beside = beside + terms[4] * padded[2:, 2:] + terms[5] * padded[:-2, 2:]
    beside = beside + terms[6] * padded[2:, :-2] + terms[7] * padded[:-2, :-2]
    return oceanf * (diag_total * field - beside)


def reference(right_side, couplings, center, ocean_mask):
    oceanf = ocean_mask.astype(jnp.float32)
    terms = coupling_terms(couplings)
    diag_total = center + terms[0] + terms[1] + terms[2] + terms[3] + terms[4] + terms[5] + terms[6] + terms[7]
    inverse = oceanf / diag_total

    def solve_one(member_rhs):
        residual = member_rhs * oceanf
        precond = residual * inverse
        direction = precond
        rz_now = jnp.sum(residual * precond)
        solution = jnp.zeros_like(residual)
        for iteration in range(ITERS):
            image_field = operate(direction, terms, diag_total, oceanf)
            step_size = rz_now / jnp.sum(direction * image_field)
            solution = solution + step_size * direction
            residual = residual - step_size * image_field
            precond = residual * inverse
            rz_new = jnp.sum(residual * precond)
            direction = precond + (rz_new / rz_now) * direction
            rz_now = rz_new
        return solution, residual

    solution, residual = lax.map(solve_one, right_side)
    return (solution, residual)
```

```python
import jax
import jax.numpy as jnp
from jax import lax
from jax.experimental import pallas as pl
from jax.experimental.pallas import tpu as pltpu
from jax.sharding import PartitionSpec as P

ITERS = 6
HALO = 8
SHIFT = 0.1
LAG = 0.05
OPPOSITE = (1, 0, 3, 2, 7, 6, 5, 4)
PAIRS = [(i, j) for i in range(ITERS) for j in range(i, ITERS + 1)]


def passed_along(value, axis, steps):
    count = lax.axis_size(axis)
    first, last = (max(0, -steps), min(count, count - steps))
    return lax.ppermute(value, axis, [(source, source + steps) for source in range(first, last)])


def around(value, axis, steps):
    count = lax.axis_size(axis)
    return lax.ppermute(value, axis, [(i, (i + steps) % count) for i in range(count)])


def coupling_terms(couplings):
    south_rows = passed_along(couplings[:, -1:, :], "gy", 1)
    extended = jnp.concatenate([south_rows, couplings], axis=1)
    west_column = around(extended[:, :, -1:], "gx", 1)
    widened = jnp.concatenate([west_column, extended], axis=2)
    return (
        widened[0, 1:, 1:],
        widened[0, :-1, 1:],
        widened[1, 1:, 1:],
        widened[1, 1:, :-1],
        widened[2, 1:, 1:],
        widened[2, :-1, 1:],
        widened[2, 1:, :-1],
        widened[2, :-1, :-1],
    )


def basis_kernel(members, rows, main_ref, side_ref, diag_ref, basis_ref, gram_ref, sides):
    tiles = rows // 8
    lanes = lax.broadcasted_iota(jnp.int32, (8, 128), 1)
    first, last = lanes == 0, lanes == 127

    def field(k, m):
        return main_ref.at[m] if k == 0 else basis_ref.at[k - 1, m]

    def side(k, m):
        return side_ref.at[m] if k == 0 else sides.at[k - 1, m]

    for k in range(ITERS):
        for tile in range(tiles):
            base = 8 * tile
            cm = [main_ref[members + d, base : base + 8, :] for d in range(8)]
            cs = [side_ref[members + d, base : base + 8, :] for d in range(8)]

            def east(a, b):
                return jnp.where(last, pltpu.roll(b, 127, 1), pltpu.roll(a, 127, 1))

            def west(a, b):
                return jnp.where(first, pltpu.roll(b, 1, 1), pltpu.roll(a, 1, 1))

            for d in (2, 4, 5):
                cm[d], cs[d] = west(cm[d], cs[d]), west(cs[d], cm[d])
            for d in (3, 6, 7):
                cm[d], cs[d] = east(cm[d], cs[d]), east(cs[d], cm[d])

            @pl.loop(0, members)
            def _(m):
                mids, easts, wests = [], [], []
                for get, c in ((field, cm), (side, cs)):
                    v = get(k, m)
                    mid = v[base : base + 8, :]
                    down = v[base - 1 : base + 7, :] if tile > 0 else pltpu.roll(mid, 1, 0)
                    up = v[base + 1 : base + 9, :] if tile < tiles - 1 else pltpu.roll(mid, 7, 0)
                    centre = c[0] * up + c[1] * down - SHIFT * mid
                    if k:
                        centre = centre - LAG * get(k - 1, m)[base : base + 8, :]
                    mids.append(centre)
                    easts.append(c[2] * mid + c[4] * up + c[5] * down)
                    wests.append(c[3] * mid + c[6] * up + c[7] * down)
                em, es = easts
                wm, ws = wests
                rem, res = pltpu.roll(em, 127, 1), pltpu.roll(es, 127, 1)
                rwm, rws = pltpu.roll(wm, 1, 1), pltpu.roll(ws, 1, 1)
                out = mids[0] + jnp.where(last, res, rem) + jnp.where(first, rws, rwm)
                basis_ref[k, m, base : base + 8, :] = out
                if k + 1 < ITERS:
                    out = mids[1] + jnp.where(last, rem, res) + jnp.where(first, rwm, rws)
                    sides[k, m, base : base + 8, :] = out

    @pl.loop(0, members)
    def _(m):
        sums = [None] * len(PAIRS)
        for tile in range(tiles - 2):
            base = HALO + 8 * tile
            diag = diag_ref[8 * tile : 8 * tile + 8, :]
            vs = [field(k, m)[base : base + 8, :] for k in range(ITERS + 1)]
            scaled = [diag * v for v in vs[:ITERS]]
            for n, (i, j) in enumerate(PAIRS):
                term = scaled[i] * vs[j]
                sums[n] = term if sums[n] is None else sums[n] + term
        for n in range(len(PAIRS)):
            gram_ref[n, pl.ds(m, 1), :] = jnp.sum(sums[n], axis=0, keepdims=True)


def coefficients(gram):
    def g(i, j):
        return gram[min(i, j)][max(i, j)]

    def applied(p):
        q = []
        for k in range(ITERS + 1):
            terms = []
            if k < len(p):
                terms.append((1.0 - SHIFT) * p[k])
            if 0 < k <= len(p):
                terms.append(-p[k - 1])
            if k + 1 < len(p):
                terms.append(-LAG * p[k + 1])
            if terms:
                q.append(sum(terms[1:], terms[0]))
        return q

    def inner(p, q):
        total = None
        for i, a in enumerate(p):
            row = None
            for j, b in enumerate(q):
                t = g(i, j) * b
                row = t if row is None else row + t
            t = a * row
            total = t if total is None else total + t
        return total

    one = jnp.ones_like(gram[0][0])
    z, p, x = [one], [one], []
    rz = g(0, 0)
    for iteration in range(ITERS):
        q = applied(p)
        step = rz / inner(p, q)
        x = [(x[k] if k < len(x) else 0.0) + step * p[k] for k in range(len(p))]
        z = [(z[k] if k < len(z) else 0.0) - step * q[k] for k in range(len(q))]
        if iteration + 1 < ITERS:
            rz_new = inner(z, z)
            beta = rz_new / rz
            p = [z[k] + (beta * p[k] if k < len(p) else 0.0) for k in range(len(z))]
            rz = rz_new
    return x, z


def combine_kernel(members, rows, z_ref, basis_ref, scale_ref, sum_ref, x_ref, r_ref, cx, cz):
    gram = [[None] * (ITERS + 1) for _ in range(ITERS + 1)]
    for n, (i, j) in enumerate(PAIRS):
        gram[i][j] = jnp.broadcast_to(sum_ref[:, n : n + 1], (members, 128))
    x, z = coefficients(gram)
    for k in range(ITERS):
        cx[k] = x[k]
    for k in range(ITERS + 1):
        cz[k] = z[k]

    @pl.loop(0, members)
    def _(m):
        xs = [jnp.broadcast_to(cx[k, pl.ds(m, 1), :], (8, 128)) for k in range(ITERS)]
        zs = [jnp.broadcast_to(cz[k, pl.ds(m, 1), :], (8, 128)) for k in range(ITERS + 1)]
        for base in range(0, rows, 8):
            at = slice(base + HALO, base + HALO + 8)
            vs = [z_ref[m, at, :]] + [basis_ref[k, m, at, :] for k in range(ITERS)]
            x_ref[m, base : base + 8, :] = sum((xs[k] * vs[k] for k in range(1, ITERS)), xs[0] * vs[0])
            total = sum((zs[k] * vs[k] for k in range(1, ITERS + 1)), zs[0] * vs[0])
            r_ref[m, base : base + 8, :] = scale_ref[base : base + 8, :] * total


def on_device(right_side, couplings, center, ocean_mask):
    members, rows, columns = right_side.shape
    oceanf = ocean_mask.astype(jnp.float32)
    terms = coupling_terms(couplings)
    diag = center + sum(terms[1:], terms[0])
    inverse = oceanf / diag
    planes = jnp.concatenate([right_side * inverse, jnp.stack(terms) * inverse], axis=0)
    edge = planes[:, -HALO:, :]
    south = passed_along(edge, "gy", 1)
    north = passed_along(planes[:, :HALO, :], "gy", -1)
    turned = jnp.concatenate([edge[:members]] + [edge[members + d][None] for d in OPPOSITE])
    turned = turned[:, ::-1, ::-1]
    count = lax.axis_size("gx")
    folded = lax.ppermute(turned, "gx", [(i, count - 1 - i) for i in range(count)])
    top = lax.axis_index("gy") == lax.axis_size("gy") - 1
    north = jnp.where(top, folded, north)
    main = jnp.concatenate([south, planes, north], axis=1)
    total = rows + 2 * HALO
    west = around(jnp.transpose(main[:, :, -HALO:], (2, 0, 1)), "gx", 1)
    east = around(jnp.transpose(main[:, :, :HALO], (2, 0, 1)), "gx", -1)
    gap = jnp.zeros((members + 8, total, columns - 2 * HALO), jnp.float32)
    side = jnp.concatenate(
        [jnp.transpose(east, (1, 2, 0)), gap, jnp.transpose(west, (1, 2, 0))], axis=2
    )
    vmem = pl.BlockSpec(memory_space=pltpu.VMEM)

    def first(*refs):
        basis_kernel(members, total, *refs)

    basis, gram = pl.pallas_call(
        first,
        out_shape=(
            jax.ShapeDtypeStruct((ITERS, members, total, columns), jnp.float32),
            jax.ShapeDtypeStruct((len(PAIRS), members, columns), jnp.float32),
        ),
        in_specs=[vmem] * 3,
        out_specs=(vmem, vmem),
        scratch_shapes=[pltpu.VMEM((ITERS - 1, members, total, columns), jnp.float32)],
    )(main, side, diag)
    sums = lax.psum(jnp.sum(gram, axis=2).T, ("gy", "gx"))

    def second(*refs):
        combine_kernel(members, rows, *refs)

    return pl.pallas_call(
        second,
        out_shape=(jax.ShapeDtypeStruct(right_side.shape, jnp.float32),) * 2,
        in_specs=[vmem] * 4,
        out_specs=(vmem, vmem),
        scratch_shapes=[
            pltpu.VMEM((ITERS, members, columns), jnp.float32),
            pltpu.VMEM((ITERS + 1, members, columns), jnp.float32),
        ],
    )(main, basis, oceanf * diag, sums)


def solution(mesh):
    in_specs = (P(None, "gy", "gx"), P(None, "gy", "gx"), P("gy", "gx"), P("gy", "gx"))
    out_specs = (P(None, "gy", "gx"), P(None, "gy", "gx"))
    return jax.shard_map(
        on_device, mesh=mesh, in_specs=in_specs, out_specs=out_specs, check_vma=False
    )
```

```python
import jax
import jax.numpy as jnp
from jax import lax
from jax.experimental import pallas as pl
from jax.experimental.pallas import tpu as pltpu
from jax.sharding import PartitionSpec as P

ITERS = 6
HALO = 8
SHIFT = 0.1
LAG = 0.05
TOGETHER = 4
OPPOSITE = (1, 0, 3, 2, 7, 6, 5, 4)
PAIRS = [(i, j) for i in range(ITERS) for j in range(i, ITERS + 1)]


def passed_along(value, axis, steps):
    count = lax.axis_size(axis)
    first, last = (max(0, -steps), min(count, count - steps))
    return lax.ppermute(value, axis, [(source, source + steps) for source in range(first, last)])


def around(value, axis, steps):
    count = lax.axis_size(axis)
    return lax.ppermute(value, axis, [(i, (i + steps) % count) for i in range(count)])


def coupling_terms(couplings):
    south_rows = passed_along(couplings[:, -1:, :], "gy", 1)
    extended = jnp.concatenate([south_rows, couplings], axis=1)
    west_column = around(extended[:, :, -1:], "gx", 1)
    widened = jnp.concatenate([west_column, extended], axis=2)
    return (
        widened[0, 1:, 1:],
        widened[0, :-1, 1:],
        widened[1, 1:, 1:],
        widened[1, 1:, :-1],
        widened[2, 1:, 1:],
        widened[2, :-1, 1:],
        widened[2, 1:, :-1],
        widened[2, :-1, :-1],
    )


def basis_kernel(members, rows, main_ref, side_ref, diag_ref, basis_ref, gram_ref, sides, gram):
    tiles = rows // 8
    lanes = lax.broadcasted_iota(jnp.int32, (8, 128), 1)
    first, last = lanes == 0, lanes == 127

    def field(k, m):
        return main_ref.at[m] if k == 0 else basis_ref.at[k - 1, m]

    def side(k, m):
        return side_ref.at[m] if k == 0 else sides.at[k - 1, m]

    for k in range(ITERS):
        for tile in range(tiles):
            base = 8 * tile
            cm = [main_ref[members + d, base : base + 8, :] for d in range(8)]
            cs = [side_ref[members + d, base : base + 8, :] for d in range(8)]

            def east(a, b):
                return jnp.where(last, pltpu.roll(b, 127, 1), pltpu.roll(a, 127, 1))

            def west(a, b):
                return jnp.where(first, pltpu.roll(b, 1, 1), pltpu.roll(a, 1, 1))

            for d in (2, 4, 5):
                cm[d], cs[d] = west(cm[d], cs[d]), west(cs[d], cm[d])
            for d in (3, 6, 7):
                cm[d], cs[d] = east(cm[d], cs[d]), east(cs[d], cm[d])

            @pl.loop(0, members // TOGETHER)
            def _(block):
                outs = []
                for within in range(TOGETHER):
                    m = block * TOGETHER + within
                    mids, easts, wests = [], [], []
                    for get, c in ((field, cm), (side, cs)):
                        v = get(k, m)
                        mid = v[base : base + 8, :]
                        down = v[base - 1 : base + 7, :] if tile > 0 else pltpu.roll(mid, 1, 0)
                        up = v[base + 1 : base + 9, :] if tile < tiles - 1 else pltpu.roll(mid, 7, 0)
                        centre = c[0] * up + c[1] * down - SHIFT * mid
                        if k:
                            centre = centre - LAG * get(k - 1, m)[base : base + 8, :]
                        mids.append(centre)
                        easts.append(c[2] * mid + c[4] * up + c[5] * down)
                        wests.append(c[3] * mid + c[6] * up + c[7] * down)
                    rem, res = [pltpu.roll(e, 127, 1) for e in easts]
                    rwm, rws = [pltpu.roll(w, 1, 1) for w in wests]
                    out_main = mids[0] + jnp.where(last, res, rem) + jnp.where(first, rws, rwm)
                    out_side = mids[1] + jnp.where(last, rem, res) + jnp.where(first, rwm, rws)
                    outs.append((m, out_main, out_side))
                for m, out_main, out_side in outs:
                    basis_ref[k, m, base : base + 8, :] = out_main
                    if k + 1 < ITERS:
                        sides[k, m, base : base + 8, :] = out_side

    @pl.loop(0, members)
    def _(m):
        sums = [None] * len(PAIRS)
        for tile in range(tiles - 2):
            base = HALO + 8 * tile
            diag = diag_ref[8 * tile : 8 * tile + 8, :]
            vs = [field(k, m)[base : base + 8, :] for k in range(ITERS + 1)]
            scaled = [diag * v for v in vs[:ITERS]]
            for n, (i, j) in enumerate(PAIRS):
                term = scaled[i] * vs[j]
                sums[n] = term if sums[n] is None else sums[n] + term
        for n in range(len(PAIRS)):
            gram[n, pl.ds(m, 1), :] = jnp.sum(sums[n], axis=0, keepdims=True)

    wide = lax.broadcasted_iota(jnp.int32, (members, 128), 1)
    packed = jnp.zeros((members, 128), jnp.float32)
    for n in range(len(PAIRS)):
        packed = jnp.where(wide == n, jnp.sum(gram[n], axis=1, keepdims=True), packed)
    gram_ref[...] = packed_in(packed)


def packed_in(values):
    members = values.shape[0]
    groups = members // 8
    width = 128 // groups
    total = values[0:8]
    for g in range(1, groups):
        total = total + pltpu.roll(values[8 * g : 8 * g + 8], width * g, 1)
    return total


def unpacked(values, members):
    groups = members // 8
    width = 128 // groups
    parts = [values] + [pltpu.roll(values, 128 - width * g, 1) for g in range(1, groups)]
    return jnp.concatenate(parts, axis=0)


def total_kernel(axes, counts, in_ref, out_ref, *scratch):
    buffers, held = scratch[: len(axes)], scratch[len(axes)]
    send_sems, recv_sems = scratch[len(axes) + 1 : 2 * len(axes) + 1], scratch[2 * len(axes) + 1 :]
    barrier = pltpu.get_barrier_semaphore()
    for axis, count in zip(axes, counts):
        me = lax.axis_index(axis)
        for step in range(1, count):
            peer = lax.rem(me + step, count)
            pl.semaphore_signal(
                barrier, inc=1, device_id={axis: peer}, device_id_type=pl.DeviceIdType.MESH
            )
    pl.semaphore_wait(barrier, sum(counts) - len(counts))
    for stage, (axis, count) in enumerate(zip(axes, counts)):
        me = lax.axis_index(axis)
        source = in_ref if stage == 0 else held
        copies = []
        for step in range(1, count):
            peer = lax.rem(me + step, count)
            copy = pltpu.make_async_remote_copy(
                src_ref=source,
                dst_ref=buffers[stage].at[step],
                send_sem=send_sems[stage].at[step],
                recv_sem=recv_sems[stage].at[step],
                device_id={axis: peer},
                device_id_type=pl.DeviceIdType.MESH,
            )
            copy.start()
            copies.append(copy)
        for copy in copies:
            copy.wait()
        total = source[...]
        for step in range(1, count):
            total = total + buffers[stage][step]
        if stage + 1 < len(axes):
            held[...] = total
        else:
            out_ref[...] = total


def coefficients(gram):
    def g(i, j):
        return gram[min(i, j)][max(i, j)]

    def applied(p):
        q = []
        for k in range(ITERS + 1):
            terms = []
            if k < len(p):
                terms.append((1.0 - SHIFT) * p[k])
            if 0 < k <= len(p):
                terms.append(-p[k - 1])
            if k + 1 < len(p):
                terms.append(-LAG * p[k + 1])
            if terms:
                q.append(sum(terms[1:], terms[0]))
        return q

    def inner(p, q):
        total = None
        for i, a in enumerate(p):
            row = None
            for j, b in enumerate(q):
                t = g(i, j) * b
                row = t if row is None else row + t
            t = a * row
            total = t if total is None else total + t
        return total

    one = jnp.ones_like(gram[0][0])
    z, p, x = [one], [one], []
    rz = g(0, 0)
    for iteration in range(ITERS):
        q = applied(p)
        step = rz / inner(p, q)
        x = [(x[k] if k < len(x) else 0.0) + step * p[k] for k in range(len(p))]
        z = [(z[k] if k < len(z) else 0.0) - step * q[k] for k in range(len(q))]
        if iteration + 1 < ITERS:
            rz_new = inner(z, z)
            beta = rz_new / rz
            p = [z[k] + (beta * p[k] if k < len(p) else 0.0) for k in range(len(z))]
            rz = rz_new
    return x, z


def combine_kernel(members, rows, z_ref, basis_ref, scale_ref, sum_ref, x_ref, r_ref, cx, cz):
    gram = [[None] * (ITERS + 1) for _ in range(ITERS + 1)]
    sums = unpacked(sum_ref[...], members)
    for n, (i, j) in enumerate(PAIRS):
        gram[i][j] = jnp.broadcast_to(sums[:, n : n + 1], (members, 128))
    x, z = coefficients(gram)
    for k in range(ITERS):
        cx[k] = x[k]
    for k in range(ITERS + 1):
        cz[k] = z[k]

    @pl.loop(0, members)
    def _(m):
        xs = [jnp.broadcast_to(cx[k, pl.ds(m, 1), :], (8, 128)) for k in range(ITERS)]
        zs = [jnp.broadcast_to(cz[k, pl.ds(m, 1), :], (8, 128)) for k in range(ITERS + 1)]
        for base in range(0, rows, 8):
            at = slice(base + HALO, base + HALO + 8)
            vs = [z_ref[m, at, :]] + [basis_ref[k, m, at, :] for k in range(ITERS)]
            x_ref[m, base : base + 8, :] = sum((xs[k] * vs[k] for k in range(1, ITERS)), xs[0] * vs[0])
            total = sum((zs[k] * vs[k] for k in range(1, ITERS + 1)), zs[0] * vs[0])
            r_ref[m, base : base + 8, :] = scale_ref[base : base + 8, :] * total


def totals(values):
    axes = ("gx", "gy")
    counts = [lax.axis_size(axis) for axis in axes]

    def kernel(*refs):
        total_kernel(axes, counts, *refs)

    vmem = pl.BlockSpec(memory_space=pltpu.VMEM)
    return pl.pallas_call(
        kernel,
        out_shape=jax.ShapeDtypeStruct(values.shape, jnp.float32),
        in_specs=[vmem],
        out_specs=vmem,
        scratch_shapes=[pltpu.VMEM((count,) + values.shape, jnp.float32) for count in counts]
        + [pltpu.VMEM(values.shape, jnp.float32)]
        + [pltpu.SemaphoreType.DMA((count,)) for count in counts] * 2,
        compiler_params=pltpu.CompilerParams(collective_id=0, has_side_effects=True),
    )(values)


def on_device(right_side, couplings, center, ocean_mask):
    members, rows, columns = right_side.shape
    oceanf = ocean_mask.astype(jnp.float32)
    terms = coupling_terms(couplings)
    diag = center + sum(terms[1:], terms[0])
    inverse = oceanf / diag
    planes = jnp.concatenate([right_side * inverse, jnp.stack(terms) * inverse], axis=0)
    edge = planes[:, -HALO:, :]
    south = passed_along(edge, "gy", 1)
    north = passed_along(planes[:, :HALO, :], "gy", -1)
    turned = jnp.concatenate([edge[:members]] + [edge[members + d][None] for d in OPPOSITE])
    turned = turned[:, ::-1, ::-1]
    count = lax.axis_size("gx")
    folded = lax.ppermute(turned, "gx", [(i, count - 1 - i) for i in range(count)])
    top = lax.axis_index("gy") == lax.axis_size("gy") - 1
    north = jnp.where(top, folded, north)
    main = jnp.concatenate([south, planes, north], axis=1)
    total = rows + 2 * HALO
    west = around(jnp.transpose(main[:, :, -HALO:], (2, 0, 1)), "gx", 1)
    east = around(jnp.transpose(main[:, :, :HALO], (2, 0, 1)), "gx", -1)
    gap = jnp.zeros((members + 8, total, columns - 2 * HALO), jnp.float32)
    side = jnp.concatenate(
        [jnp.transpose(east, (1, 2, 0)), gap, jnp.transpose(west, (1, 2, 0))], axis=2
    )
    vmem = pl.BlockSpec(memory_space=pltpu.VMEM)

    def first(*refs):
        basis_kernel(members, total, *refs)

    basis, gram = pl.pallas_call(
        first,
        out_shape=(
            jax.ShapeDtypeStruct((ITERS, members, total, columns), jnp.float32),
            jax.ShapeDtypeStruct((8, 128), jnp.float32),
        ),
        in_specs=[vmem] * 3,
        out_specs=(vmem, vmem),
        scratch_shapes=[
            pltpu.VMEM((ITERS - 1, members, total, columns), jnp.float32),
            pltpu.VMEM((len(PAIRS), members, columns), jnp.float32),
        ],
    )(main, side, diag)
    sums = totals(gram)

    def second(*refs):
        combine_kernel(members, rows, *refs)

    return pl.pallas_call(
        second,
        out_shape=(jax.ShapeDtypeStruct(right_side.shape, jnp.float32),) * 2,
        in_specs=[vmem] * 4,
        out_specs=(vmem, vmem),
        scratch_shapes=[
            pltpu.VMEM((ITERS, members, columns), jnp.float32),
            pltpu.VMEM((ITERS + 1, members, columns), jnp.float32),
        ],
    )(main, basis, oceanf * diag, sums)


def solution(mesh):
    in_specs = (P(None, "gy", "gx"), P(None, "gy", "gx"), P("gy", "gx"), P("gy", "gx"))
    out_specs = (P(None, "gy", "gx"), P(None, "gy", "gx"))
    return jax.shard_map(
        on_device, mesh=mesh, in_specs=in_specs, out_specs=out_specs, check_vma=False
    )
```

```python
import jax
import jax.numpy as jnp
from jax import lax
from jax.experimental import pallas as pl
from jax.experimental.pallas import tpu as pltpu
from jax.sharding import PartitionSpec as P

ITERS = 6
HALO = 8
SHIFT = 0.1
LAG = 0.05
TOGETHER = 4
OPPOSITE = (1, 0, 3, 2, 7, 6, 5, 4)
PAIRS = [(i, j) for i in range(ITERS) for j in range(i, ITERS + 1)]


def slots(lanes, g):
    return (lanes >= 8 * g) & (lanes < 8 * g + 8)


def reversed_tile(x, lanes, subs):
    for bit in range(7):
        step = 1 << bit
        x = jnp.where((lanes & step) == 0, pltpu.roll(x, 128 - step, 1), pltpu.roll(x, step, 1))
    for bit in range(3):
        step = 1 << bit
        x = jnp.where((subs & step) == 0, pltpu.roll(x, 8 - step, 0), pltpu.roll(x, step, 0))
    return x


def halo_kernel(
    members, ny, nx, rhs, coup, center, mask, main, strips, scale,
    from_west, from_south, from_corner, rows_s, rows_n, turned, packed, received, send, recv,
):
    rows = rhs.shape[1]
    tiles = rows // 8
    planes = members + 8
    y, x = lax.axis_index("gy"), lax.axis_index("gx")
    north, south = lax.rem(y + 1, ny), lax.rem(y + ny - 1, ny)
    east, west = lax.rem(x + 1, nx), lax.rem(x + nx - 1, nx)
    mirror = nx - 1 - x
    top, bottom = y == ny - 1, y == 0
    barrier = pltpu.get_barrier_semaphore()
    peers = ((y, east), (y, west), (north, x), (south, x), (north, east), (south, west), (y, mirror))
    for there in peers:
        pl.semaphore_signal(barrier, inc=1, device_id=there, device_id_type=pl.DeviceIdType.MESH)
    pl.semaphore_wait(barrier, len(peers))

    def copy(src, dst, n, there):
        return pltpu.make_async_remote_copy(
            src_ref=src,
            dst_ref=dst,
            send_sem=send.at[n],
            recv_sem=recv.at[n],
            device_id=there,
            device_id_type=pl.DeviceIdType.MESH,
        )

    last_rows = coup.at[:, rows - 8 : rows, :]
    copies = [
        copy(coup, from_west, 0, (y, east)),
        copy(last_rows, from_south, 1, (north, x)),
        copy(last_rows, from_corner, 2, (north, east)),
    ]
    for c in copies:
        c.start()
    lanes = lax.broadcasted_iota(jnp.int32, (8, 128), 1)
    subs = lax.broadcasted_iota(jnp.int32, (8, 128), 0)
    first = lanes == 0
    inside = jnp.where(bottom, 0.0, 1.0)
    for c in copies:
        c.wait()

    def below(ref, edge, a, t):
        if t:
            return ref[a, 8 * t - 1 : 8 * t + 7, :]
        row = jnp.broadcast_to(edge[a, 7:8, :] * inside, (8, 128))
        return jnp.where(subs == 0, row, pltpu.roll(ref[a, 0:8, :], 1, 0))

    def westward(here, beside):
        return jnp.where(first, pltpu.roll(beside, 1, 1), pltpu.roll(here, 1, 1))

    for t in range(tiles):
        at = slice(8 * t, 8 * t + 8)
        out = slice(8 * t + HALO, 8 * t + HALO + 8)
        here = [coup[a, at, :] for a in range(3)]
        prev = [below(coup, from_south, a, t) for a in range(3)]
        beside = [from_west[a, at, :] for a in range(3)]
        corner = below(from_west, from_corner, 2, t)
        terms = (
            here[0],
            prev[0],
            here[1],
            westward(here[1], beside[1]),
            here[2],
            prev[2],
            westward(here[2], beside[2]),
            westward(prev[2], corner),
        )
        diag = center[at, :] + sum(terms[1:], terms[0])
        ocean = mask[at, :].astype(jnp.float32)
        inverse = ocean / diag
        scale[at, :] = ocean * diag
        for d in range(8):
            main[members + d, out, :] = terms[d] * inverse

        @pl.loop(0, members // 8)
        def _(block):
            for within in range(8):
                m = block * 8 + within
                main[m, out, :] = rhs[m, at, :] * inverse

    up = copy(main.at[:, rows : rows + 8, :], rows_s, 3, (north, x))
    down = copy(main.at[:, 8:16, :], rows_n, 4, (south, x))
    up.start()

    @pl.when(jnp.logical_not(bottom))
    def _():
        down.start()

    @pl.when(top)
    def _():
        @pl.loop(0, members // 4)
        def _(block):
            for within in range(4):
                m = block * 4 + within
                turned[m] = reversed_tile(main[m, rows : rows + 8, :], lanes, subs)

        for d in range(8):
            tile = main[members + OPPOSITE[d], rows : rows + 8, :]
            turned[members + d] = reversed_tile(tile, lanes, subs)
        pltpu.make_async_remote_copy(
            src_ref=turned,
            dst_ref=rows_n,
            send_sem=send.at[5],
            recv_sem=recv.at[4],
            device_id=(y, mirror),
            device_id_type=pl.DeviceIdType.MESH,
        ).start()

    up.wait()
    down.wait_recv()

    @pl.when(jnp.logical_not(bottom))
    def _():
        down.wait_send()

    @pl.when(top)
    def _():
        copy(turned, rows_n, 5, (y, mirror)).wait_send()

    main[:, 0:8, :] = rows_s[...] * inside
    main[:, rows + 8 : rows + 16, :] = rows_n[...]

    @pl.loop(0, tiles + 2)
    def _(t):
        at = pl.ds(pl.multiple_of(8 * t, 8), 8)
        for group in range(3):
            eastbound = jnp.zeros((8, 128), jnp.float32)
            westbound = eastbound
            for g in range(min(16, planes - 16 * group)):
                v = main[16 * group + g, at, :]
                slot = slots(lanes, g)
                eastbound = jnp.where(slot, pltpu.roll(v, (8 * g + 8) % 128, 1), eastbound)
                westbound = jnp.where(slot, pltpu.roll(v, 8 * g, 1) if g else v, westbound)
            packed[0, group, at, :] = eastbound
            packed[1, group, at, :] = westbound

    copies = [
        copy(packed.at[0], received.at[1], 6, (y, east)),
        copy(packed.at[1], received.at[0], 7, (y, west)),
    ]
    for c in copies:
        c.start()
    for c in copies:
        c.wait()
    strips[...] = received[...]


def basis_kernel(members, rows, main_ref, strip_ref, diag_ref, basis_ref, gram_ref, sides, strip_c, gram):
    tiles = rows // 8
    lanes = lax.broadcasted_iota(jnp.int32, (8, 128), 1)
    first, last = lanes == 0, lanes == 127
    slot_first, slot_last = lanes % 8 == 0, lanes % 8 == 7

    def field(k, m):
        return main_ref.at[m] if k == 0 else basis_ref.at[k - 1, m]

    def side(k, s, group):
        return strip_ref.at[s, group] if k == 0 else sides.at[k - 1, s, group]

    for tile in range(tiles):
        at = slice(8 * tile, 8 * tile + 8)
        for d in range(8):
            for s in range(2):
                v = jnp.where(slots(lanes, d), strip_ref[s, 2, at, :], 0.0)
                for step in (8, 16, 32, 64):
                    v = v + pltpu.roll(v, step, 1)
                strip_c[s, d, at, :] = v

    def three(v, before, c, tile):
        base = 8 * tile
        mid = v[base : base + 8, :]
        down = v[base - 1 : base + 7, :] if tile > 0 else pltpu.roll(mid, 1, 0)
        up = v[base + 1 : base + 9, :] if tile < tiles - 1 else pltpu.roll(mid, 7, 0)
        centre = c[0] * up + c[1] * down - SHIFT * mid
        if before is not None:
            centre = centre - LAG * before[base : base + 8, :]
        return (
            centre,
            c[2] * mid + c[4] * up + c[5] * down,
            c[3] * mid + c[6] * up + c[7] * down,
        )

    for k in range(ITERS):
        final = k + 1 == ITERS
        for tile in range(1, tiles - 1) if final else range(tiles):
            at = slice(8 * tile, 8 * tile + 8)
            cm = [main_ref[members + d, at, :] for d in range(8)]
            ce = [strip_c[0, d, at, :] for d in range(8)]
            cw = [strip_c[1, d, at, :] for d in range(8)]
            for d in (2, 4, 5):
                edge = jnp.broadcast_to(cm[d][:, 127:128], (8, 128))
                ce[d] = jnp.where(slot_first, edge, pltpu.roll(ce[d], 1, 1))
                cm[d] = jnp.where(first, pltpu.roll(cw[d], 1, 1), pltpu.roll(cm[d], 1, 1))
                cw[d] = pltpu.roll(cw[d], 1, 1)
            for d in (3, 6, 7):
                edge = jnp.broadcast_to(cm[d][:, 0:1], (8, 128))
                cw[d] = jnp.where(slot_last, edge, pltpu.roll(cw[d], 127, 1))
                cm[d] = jnp.where(last, pltpu.roll(ce[d], 127, 1), pltpu.roll(cm[d], 127, 1))
                ce[d] = pltpu.roll(ce[d], 127, 1)

            @pl.loop(0, members // 16)
            def _(group):
                before = (lambda s: side(k - 1, s, group)) if k else (lambda s: None)
                mid_e, e_e, w_e = three(side(k, 0, group), before(0), ce, tile)
                mid_w, e_w, w_w = three(side(k, 1, group), before(1), cw, tile)
                into_e, into_w = pltpu.roll(w_e, 1, 1), pltpu.roll(e_w, 127, 1)
                for block in range(16 // TOGETHER):
                    outs = []
                    for g in range(block * TOGETHER, (block + 1) * TOGETHER):
                        m = group * 16 + g
                        mid, e, w = three(field(k, m), field(k - 1, m) if k else None, cm, tile)
                        shift_e = 127 - 8 * g
                        shift_w = (121 - 8 * g) % 128
                        out = mid + jnp.where(last, pltpu.roll(e_e, shift_e, 1), pltpu.roll(e, 127, 1))
                        out = out + jnp.where(first, pltpu.roll(w_w, shift_w, 1), pltpu.roll(w, 1, 1))
                        outs.append((m, out))
                        if not final:
                            into_e = jnp.where(lanes == 8 * g, pltpu.roll(w, 8 * g + 1, 1), into_e)
                            into_w = jnp.where(lanes == 8 * g + 7, pltpu.roll(e, 8 * g + 7, 1), into_w)
                    for m, out in outs:
                        basis_ref[k, m, at, :] = out
                if not final:
                    sides[k, 0, group, at, :] = mid_e + pltpu.roll(e_e, 127, 1) + into_e
                    sides[k, 1, group, at, :] = mid_w + pltpu.roll(w_w, 1, 1) + into_w

    @pl.loop(0, members)
    def _(m):
        sums = [None] * len(PAIRS)
        for tile in range(tiles - 2):
            base = HALO + 8 * tile
            diag = diag_ref[8 * tile : 8 * tile + 8, :]
            vs = [field(k, m)[base : base + 8, :] for k in range(ITERS + 1)]
            scaled = [diag * v for v in vs[:ITERS]]
            for n, (i, j) in enumerate(PAIRS):
                term = scaled[i] * vs[j]
                sums[n] = term if sums[n] is None else sums[n] + term
        for n in range(len(PAIRS)):
            gram[n, pl.ds(m, 1), :] = jnp.sum(sums[n], axis=0, keepdims=True)

    wide = lax.broadcasted_iota(jnp.int32, (members, 128), 1)
    packed = jnp.zeros((members, 128), jnp.float32)
    for n in range(len(PAIRS)):
        packed = jnp.where(wide == n, jnp.sum(gram[n], axis=1, keepdims=True), packed)
    gram_ref[...] = packed_in(packed)


def packed_in(values):
    members = values.shape[0]
    groups = members // 8
    width = 128 // groups
    total = values[0:8]
    for g in range(1, groups):
        total = total + pltpu.roll(values[8 * g : 8 * g + 8], width * g, 1)
    return total


def unpacked(values, members):
    groups = members // 8
    width = 128 // groups
    parts = [values] + [pltpu.roll(values, 128 - width * g, 1) for g in range(1, groups)]
    return jnp.concatenate(parts, axis=0)


def total_kernel(axes, counts, in_ref, out_ref, *scratch):
    buffers, held = scratch[: len(axes)], scratch[len(axes)]
    send_sems, recv_sems = scratch[len(axes) + 1 : 2 * len(axes) + 1], scratch[2 * len(axes) + 1 :]
    barrier = pltpu.get_barrier_semaphore()
    for axis, count in zip(axes, counts):
        me = lax.axis_index(axis)
        for step in range(1, count):
            peer = lax.rem(me + step, count)
            pl.semaphore_signal(
                barrier, inc=1, device_id={axis: peer}, device_id_type=pl.DeviceIdType.MESH
            )
    pl.semaphore_wait(barrier, sum(counts) - len(counts))
    for stage, (axis, count) in enumerate(zip(axes, counts)):
        me = lax.axis_index(axis)
        source = in_ref if stage == 0 else held
        copies = []
        for step in range(1, count):
            peer = lax.rem(me + step, count)
            copy = pltpu.make_async_remote_copy(
                src_ref=source,
                dst_ref=buffers[stage].at[step],
                send_sem=send_sems[stage].at[step],
                recv_sem=recv_sems[stage].at[step],
                device_id={axis: peer},
                device_id_type=pl.DeviceIdType.MESH,
            )
            copy.start()
            copies.append(copy)
        for copy in copies:
            copy.wait()
        total = source[...]
        for step in range(1, count):
            total = total + buffers[stage][step]
        if stage + 1 < len(axes):
            held[...] = total
        else:
            out_ref[...] = total


def coefficients(gram):
    def g(i, j):
        return gram[min(i, j)][max(i, j)]

    def applied(p):
        q = []
        for k in range(ITERS + 1):
            terms = []
            if k < len(p):
                terms.append((1.0 - SHIFT) * p[k])
            if 0 < k <= len(p):
                terms.append(-p[k - 1])
            if k + 1 < len(p):
                terms.append(-LAG * p[k + 1])
            if terms:
                q.append(sum(terms[1:], terms[0]))
        return q

    def inner(p, q):
        total = None
        for i, a in enumerate(p):
            row = None
            for j, b in enumerate(q):
                t = g(i, j) * b
                row = t if row is None else row + t
            t = a * row
            total = t if total is None else total + t
        return total

    one = jnp.ones_like(gram[0][0])
    z, p, x = [one], [one], []
    rz = g(0, 0)
    for iteration in range(ITERS):
        q = applied(p)
        step = rz / inner(p, q)
        x = [(x[k] if k < len(x) else 0.0) + step * p[k] for k in range(len(p))]
        z = [(z[k] if k < len(z) else 0.0) - step * q[k] for k in range(len(q))]
        if iteration + 1 < ITERS:
            rz_new = inner(z, z)
            beta = rz_new / rz
            p = [z[k] + (beta * p[k] if k < len(p) else 0.0) for k in range(len(z))]
            rz = rz_new
    return x, z


def combine_kernel(members, rows, z_ref, basis_ref, scale_ref, sum_ref, x_ref, r_ref, cx, cz):
    gram = [[None] * (ITERS + 1) for _ in range(ITERS + 1)]
    sums = unpacked(sum_ref[...], members)
    for n, (i, j) in enumerate(PAIRS):
        gram[i][j] = jnp.broadcast_to(sums[:, n : n + 1], (members, 128))
    x, z = coefficients(gram)
    for k in range(ITERS):
        cx[k] = x[k]
    for k in range(ITERS + 1):
        cz[k] = z[k]

    @pl.loop(0, members)
    def _(m):
        xs = [jnp.broadcast_to(cx[k, pl.ds(m, 1), :], (8, 128)) for k in range(ITERS)]
        zs = [jnp.broadcast_to(cz[k, pl.ds(m, 1), :], (8, 128)) for k in range(ITERS + 1)]
        for base in range(0, rows, 8):
            at = slice(base + HALO, base + HALO + 8)
            vs = [z_ref[m, at, :]] + [basis_ref[k, m, at, :] for k in range(ITERS)]
            x_ref[m, base : base + 8, :] = sum((xs[k] * vs[k] for k in range(1, ITERS)), xs[0] * vs[0])
            total = sum((zs[k] * vs[k] for k in range(1, ITERS + 1)), zs[0] * vs[0])
            r_ref[m, base : base + 8, :] = scale_ref[base : base + 8, :] * total


def totals(values):
    axes = ("gx", "gy")
    counts = [lax.axis_size(axis) for axis in axes]

    def kernel(*refs):
        total_kernel(axes, counts, *refs)

    vmem = pl.BlockSpec(memory_space=pltpu.VMEM)
    return pl.pallas_call(
        kernel,
        out_shape=jax.ShapeDtypeStruct(values.shape, jnp.float32),
        in_specs=[vmem],
        out_specs=vmem,
        scratch_shapes=[pltpu.VMEM((count,) + values.shape, jnp.float32) for count in counts]
        + [pltpu.VMEM(values.shape, jnp.float32)]
        + [pltpu.SemaphoreType.DMA((count,)) for count in counts] * 2,
        compiler_params=pltpu.CompilerParams(collective_id=0, has_side_effects=True),
    )(values)


def on_device(right_side, couplings, center, ocean_mask):
    members, rows, columns = right_side.shape
    total = rows + 2 * HALO
    planes = members + 8
    ny, nx = lax.axis_size("gy"), lax.axis_size("gx")
    vmem = pl.BlockSpec(memory_space=pltpu.VMEM)
    f32 = jnp.float32

    def halo(*refs):
        halo_kernel(members, ny, nx, *refs)

    main, strips, scale = pl.pallas_call(
        halo,
        out_shape=(
            jax.ShapeDtypeStruct((planes, total, columns), f32),
            jax.ShapeDtypeStruct((2, 3, total, columns), f32),
            jax.ShapeDtypeStruct((rows, columns), f32),
        ),
        in_specs=[vmem] * 4,
        out_specs=(vmem,) * 3,
        scratch_shapes=[
            pltpu.VMEM((3, rows, columns), f32),
            pltpu.VMEM((3, 8, columns), f32),
            pltpu.VMEM((3, 8, columns), f32),
            pltpu.VMEM((planes, 8, columns), f32),
            pltpu.VMEM((planes, 8, columns), f32),
            pltpu.VMEM((planes, 8, columns), f32),
            pltpu.VMEM((2, 3, total, columns), f32),
            pltpu.VMEM((2, 3, total, columns), f32),
            pltpu.SemaphoreType.DMA((8,)),
            pltpu.SemaphoreType.DMA((8,)),
        ],
        compiler_params=pltpu.CompilerParams(collective_id=1, has_side_effects=True),
    )(right_side, couplings, center, ocean_mask)

    def first(*refs):
        basis_kernel(members, total, *refs)

    basis, gram = pl.pallas_call(
        first,
        out_shape=(
            jax.ShapeDtypeStruct((ITERS, members, total, columns), f32),
            jax.ShapeDtypeStruct((8, 128), f32),
        ),
        in_specs=[vmem] * 3,
        out_specs=(vmem, vmem),
        scratch_shapes=[
            pltpu.VMEM((ITERS - 1, 2, 2, total, columns), f32),
            pltpu.VMEM((2, 8, total, columns), f32),
            pltpu.VMEM((len(PAIRS), members, columns), f32),
        ],
    )(main, strips, scale)
    sums = totals(gram)

    def second(*refs):
        combine_kernel(members, rows, *refs)

    return pl.pallas_call(
        second,
        out_shape=(jax.ShapeDtypeStruct(right_side.shape, jnp.float32),) * 2,
        in_specs=[vmem] * 4,
        out_specs=(vmem, vmem),
        scratch_shapes=[
            pltpu.VMEM((ITERS, members, columns), jnp.float32),
            pltpu.VMEM((ITERS + 1, members, columns), jnp.float32),
        ],
    )(main, basis, scale, sums)


def solution(mesh):
    in_specs = (P(None, "gy", "gx"), P(None, "gy", "gx"), P("gy", "gx"), P("gy", "gx"))
    out_specs = (P(None, "gy", "gx"), P(None, "gy", "gx"))
    return jax.shard_map(
        on_device, mesh=mesh, in_specs=in_specs, out_specs=out_specs, check_vma=False
    )
```

```python
import jax
import jax.numpy as jnp
from jax import lax
from jax.experimental import pallas as pl
from jax.experimental.pallas import tpu as pltpu
from jax.sharding import PartitionSpec as P

ITERS = 6
HALO = 8
SHIFT = 0.1
LAG = 0.05
TOGETHER = 8
GRANT = 20 * 1024 * 1024
OPPOSITE = (1, 0, 3, 2, 7, 6, 5, 4)
PAIRS = [(i, j) for i in range(ITERS) for j in range(i, ITERS + 1)]


def slots(lanes, g):
    return (lanes >= 8 * g) & (lanes < 8 * g + 8)


def reversed_tile(x, lanes, subs):
    for bit in range(7):
        step = 1 << bit
        x = jnp.where((lanes & step) == 0, pltpu.roll(x, 128 - step, 1), pltpu.roll(x, step, 1))
    for bit in range(3):
        step = 1 << bit
        x = jnp.where((subs & step) == 0, pltpu.roll(x, 8 - step, 0), pltpu.roll(x, step, 0))
    return x


def halo_kernel(
    members, ny, nx, rhs, coup, center, mask, main, strips, scale,
    from_west, from_south, from_corner, rows_s, rows_n, turned, packed, received, send, recv,
):
    rows = rhs.shape[1]
    tiles = rows // 8
    planes = members + 8
    y, x = lax.axis_index("gy"), lax.axis_index("gx")
    north, south = lax.rem(y + 1, ny), lax.rem(y + ny - 1, ny)
    east, west = lax.rem(x + 1, nx), lax.rem(x + nx - 1, nx)
    mirror = nx - 1 - x
    top, bottom = y == ny - 1, y == 0
    barrier = pltpu.get_barrier_semaphore()
    peers = ((y, east), (y, west), (north, x), (south, x), (north, east), (south, west), (y, mirror))
    for there in peers:
        pl.semaphore_signal(barrier, inc=1, device_id=there, device_id_type=pl.DeviceIdType.MESH)
    pl.semaphore_wait(barrier, len(peers))

    def copy(src, dst, n, there):
        return pltpu.make_async_remote_copy(
            src_ref=src,
            dst_ref=dst,
            send_sem=send.at[n],
            recv_sem=recv.at[n],
            device_id=there,
            device_id_type=pl.DeviceIdType.MESH,
        )

    last_rows = coup.at[:, rows - 8 : rows, :]
    copies = [
        copy(coup, from_west, 0, (y, east)),
        copy(last_rows, from_south, 1, (north, x)),
        copy(last_rows, from_corner, 2, (north, east)),
    ]
    for c in copies:
        c.start()
    lanes = lax.broadcasted_iota(jnp.int32, (8, 128), 1)
    subs = lax.broadcasted_iota(jnp.int32, (8, 128), 0)
    first = lanes == 0
    inside = jnp.where(bottom, 0.0, 1.0)
    for c in copies:
        c.wait()

    def below(ref, edge, a, t):
        if t:
            return ref[a, 8 * t - 1 : 8 * t + 7, :]
        row = jnp.broadcast_to(edge[a, 7:8, :] * inside, (8, 128))
        return jnp.where(subs == 0, row, pltpu.roll(ref[a, 0:8, :], 1, 0))

    def westward(here, beside):
        return jnp.where(first, pltpu.roll(beside, 1, 1), pltpu.roll(here, 1, 1))

    for t in range(tiles):
        at = slice(8 * t, 8 * t + 8)
        out = slice(8 * t + HALO, 8 * t + HALO + 8)
        here = [coup[a, at, :] for a in range(3)]
        prev = [below(coup, from_south, a, t) for a in range(3)]
        beside = [from_west[a, at, :] for a in range(3)]
        corner = below(from_west, from_corner, 2, t)
        terms = (
            here[0],
            prev[0],
            here[1],
            westward(here[1], beside[1]),
            here[2],
            prev[2],
            westward(here[2], beside[2]),
            westward(prev[2], corner),
        )
        diag = center[at, :] + sum(terms[1:], terms[0])
        ocean = mask[at, :].astype(jnp.float32)
        inverse = ocean / diag
        scale[at, :] = ocean * diag
        for d in range(8):
            main[members + d, out, :] = terms[d] * inverse

        @pl.loop(0, members // 8)
        def _(block):
            for within in range(8):
                m = block * 8 + within
                main[m, out, :] = rhs[m, at, :] * inverse

    up = copy(main.at[:, rows : rows + 8, :], rows_s, 3, (north, x))
    down = copy(main.at[:, 8:16, :], rows_n, 4, (south, x))
    up.start()

    @pl.when(jnp.logical_not(bottom))
    def _():
        down.start()

    @pl.when(top)
    def _():
        @pl.loop(0, members // 4)
        def _(block):
            for within in range(4):
                m = block * 4 + within
                turned[m] = reversed_tile(main[m, rows : rows + 8, :], lanes, subs)

        for d in range(8):
            tile = main[members + OPPOSITE[d], rows : rows + 8, :]
            turned[members + d] = reversed_tile(tile, lanes, subs)
        pltpu.make_async_remote_copy(
            src_ref=turned,
            dst_ref=rows_n,
            send_sem=send.at[5],
            recv_sem=recv.at[4],
            device_id=(y, mirror),
            device_id_type=pl.DeviceIdType.MESH,
        ).start()

    up.wait()
    down.wait_recv()

    @pl.when(jnp.logical_not(bottom))
    def _():
        down.wait_send()

    @pl.when(top)
    def _():
        copy(turned, rows_n, 5, (y, mirror)).wait_send()

    main[:, 0:8, :] = rows_s[...] * inside
    main[:, rows + 8 : rows + 16, :] = rows_n[...]

    @pl.loop(0, tiles + 2)
    def _(t):
        at = pl.ds(pl.multiple_of(8 * t, 8), 8)
        for group in range(3):
            eastbound = jnp.zeros((8, 128), jnp.float32)
            westbound = eastbound
            for g in range(min(16, planes - 16 * group)):
                v = main[16 * group + g, at, :]
                slot = slots(lanes, g)
                eastbound = jnp.where(slot, pltpu.roll(v, (8 * g + 8) % 128, 1), eastbound)
                westbound = jnp.where(slot, pltpu.roll(v, 8 * g, 1) if g else v, westbound)
            packed[0, group, at, :] = eastbound
            packed[1, group, at, :] = westbound

    copies = [
        copy(packed.at[0], received.at[1], 6, (y, east)),
        copy(packed.at[1], received.at[0], 7, (y, west)),
    ]
    for c in copies:
        c.start()
    for c in copies:
        c.wait()
    strips[...] = received[...]


def basis_kernel(members, rows, main_ref, strip_ref, diag_ref, *refs):
    basis, gram_ref = refs[:ITERS], refs[ITERS]
    sides, (strip_c, gram) = refs[ITERS + 1 : 2 * ITERS], refs[2 * ITERS :]
    tiles = rows // 8
    lanes = lax.broadcasted_iota(jnp.int32, (8, 128), 1)
    first, last = lanes == 0, lanes == 127
    slot_first, slot_last = lanes % 8 == 0, lanes % 8 == 7

    def field(k, m):
        return main_ref.at[m] if k == 0 else basis[k - 1].at[m]

    def side(k, s, group):
        return strip_ref.at[s, group] if k == 0 else sides[k - 1].at[s, group]

    for tile in range(tiles):
        at = slice(8 * tile, 8 * tile + 8)
        for d in range(8):
            for s in range(2):
                v = jnp.where(slots(lanes, d), strip_ref[s, 2, at, :], 0.0)
                for step in (8, 16, 32, 64):
                    v = v + pltpu.roll(v, step, 1)
                strip_c[s, d, at, :] = v

    def three(v, before, c, tile):
        base = 8 * tile
        mid = v[base : base + 8, :]
        down = v[base - 1 : base + 7, :] if tile > 0 else pltpu.roll(mid, 1, 0)
        up = v[base + 1 : base + 9, :] if tile < tiles - 1 else pltpu.roll(mid, 7, 0)
        centre = c[0] * up + c[1] * down - SHIFT * mid
        if before is not None:
            centre = centre - LAG * before[base : base + 8, :]
        return (
            centre,
            c[2] * mid + c[4] * up + c[5] * down,
            c[3] * mid + c[6] * up + c[7] * down,
        )

    for k in range(ITERS):
        final = k + 1 == ITERS
        for tile in range(1, tiles - 1) if final else range(tiles):
            at = slice(8 * tile, 8 * tile + 8)
            cm = [main_ref[members + d, at, :] for d in range(8)]
            ce = [strip_c[0, d, at, :] for d in range(8)]
            cw = [strip_c[1, d, at, :] for d in range(8)]
            for d in (2, 4, 5):
                edge = jnp.broadcast_to(cm[d][:, 127:128], (8, 128))
                ce[d] = jnp.where(slot_first, edge, pltpu.roll(ce[d], 1, 1))
                cm[d] = jnp.where(first, pltpu.roll(cw[d], 1, 1), pltpu.roll(cm[d], 1, 1))
                cw[d] = pltpu.roll(cw[d], 1, 1)
            for d in (3, 6, 7):
                edge = jnp.broadcast_to(cm[d][:, 0:1], (8, 128))
                cw[d] = jnp.where(slot_last, edge, pltpu.roll(cw[d], 127, 1))
                cm[d] = jnp.where(last, pltpu.roll(ce[d], 127, 1), pltpu.roll(cm[d], 127, 1))
                ce[d] = pltpu.roll(ce[d], 127, 1)

            @pl.loop(0, members // 16)
            def _(group):
                before = (lambda s: side(k - 1, s, group)) if k else (lambda s: None)
                mid_e, e_e, w_e = three(side(k, 0, group), before(0), ce, tile)
                mid_w, e_w, w_w = three(side(k, 1, group), before(1), cw, tile)
                into_e, into_w = pltpu.roll(w_e, 1, 1), pltpu.roll(e_w, 127, 1)
                for block in range(16 // TOGETHER):
                    outs = []
                    for g in range(block * TOGETHER, (block + 1) * TOGETHER):
                        m = group * 16 + g
                        mid, e, w = three(field(k, m), field(k - 1, m) if k else None, cm, tile)
                        shift_e = 127 - 8 * g
                        shift_w = (121 - 8 * g) % 128
                        out = mid + jnp.where(last, pltpu.roll(e_e, shift_e, 1), pltpu.roll(e, 127, 1))
                        out = out + jnp.where(first, pltpu.roll(w_w, shift_w, 1), pltpu.roll(w, 1, 1))
                        outs.append((m, out))
                        if not final:
                            into_e = jnp.where(lanes == 8 * g, pltpu.roll(w, 8 * g + 1, 1), into_e)
                            into_w = jnp.where(lanes == 8 * g + 7, pltpu.roll(e, 8 * g + 7, 1), into_w)
                    for m, out in outs:
                        basis[k][m, at, :] = out
                if not final:
                    sides[k][0, group, at, :] = mid_e + pltpu.roll(e_e, 127, 1) + into_e
                    sides[k][1, group, at, :] = mid_w + pltpu.roll(w_w, 1, 1) + into_w

    @pl.loop(0, members)
    def _(m):
        sums = [None] * len(PAIRS)
        for tile in range(tiles - 2):
            base = HALO + 8 * tile
            diag = diag_ref[8 * tile : 8 * tile + 8, :]
            vs = [field(k, m)[base : base + 8, :] for k in range(ITERS + 1)]
            scaled = [diag * v for v in vs[:ITERS]]
            for n, (i, j) in enumerate(PAIRS):
                term = scaled[i] * vs[j]
                sums[n] = term if sums[n] is None else sums[n] + term
        for n in range(len(PAIRS)):
            gram[n, pl.ds(m, 1), :] = jnp.sum(sums[n], axis=0, keepdims=True)

    wide = lax.broadcasted_iota(jnp.int32, (members, 128), 1)
    packed = jnp.zeros((members, 128), jnp.float32)
    for n in range(len(PAIRS)):
        packed = jnp.where(wide == n, jnp.sum(gram[n], axis=1, keepdims=True), packed)
    gram_ref[...] = packed_in(packed)


def packed_in(values):
    members = values.shape[0]
    groups = members // 8
    width = 128 // groups
    total = values[0:8]
    for g in range(1, groups):
        total = total + pltpu.roll(values[8 * g : 8 * g + 8], width * g, 1)
    return total


def unpacked(values, members):
    groups = members // 8
    width = 128 // groups
    parts = [values] + [pltpu.roll(values, 128 - width * g, 1) for g in range(1, groups)]
    return jnp.concatenate(parts, axis=0)


def total_kernel(axes, counts, in_ref, out_ref, *scratch):
    buffers, held = scratch[: len(axes)], scratch[len(axes)]
    send_sems, recv_sems = scratch[len(axes) + 1 : 2 * len(axes) + 1], scratch[2 * len(axes) + 1 :]
    barrier = pltpu.get_barrier_semaphore()
    for axis, count in zip(axes, counts):
        me = lax.axis_index(axis)
        for step in range(1, count):
            peer = lax.rem(me + step, count)
            pl.semaphore_signal(
                barrier, inc=1, device_id={axis: peer}, device_id_type=pl.DeviceIdType.MESH
            )
    pl.semaphore_wait(barrier, sum(counts) - len(counts))
    for stage, (axis, count) in enumerate(zip(axes, counts)):
        me = lax.axis_index(axis)
        source = in_ref if stage == 0 else held
        copies = []
        for step in range(1, count):
            peer = lax.rem(me + step, count)
            copy = pltpu.make_async_remote_copy(
                src_ref=source,
                dst_ref=buffers[stage].at[step],
                send_sem=send_sems[stage].at[step],
                recv_sem=recv_sems[stage].at[step],
                device_id={axis: peer},
                device_id_type=pl.DeviceIdType.MESH,
            )
            copy.start()
            copies.append(copy)
        for copy in copies:
            copy.wait()
        total = source[...]
        for step in range(1, count):
            total = total + buffers[stage][step]
        if stage + 1 < len(axes):
            held[...] = total
        else:
            out_ref[...] = total


def coefficients(gram):
    def g(i, j):
        return gram[min(i, j)][max(i, j)]

    def applied(p):
        q = []
        for k in range(ITERS + 1):
            terms = []
            if k < len(p):
                terms.append((1.0 - SHIFT) * p[k])
            if 0 < k <= len(p):
                terms.append(-p[k - 1])
            if k + 1 < len(p):
                terms.append(-LAG * p[k + 1])
            if terms:
                q.append(sum(terms[1:], terms[0]))
        return q

    def inner(p, q):
        total = None
        for i, a in enumerate(p):
            row = None
            for j, b in enumerate(q):
                t = g(i, j) * b
                row = t if row is None else row + t
            t = a * row
            total = t if total is None else total + t
        return total

    one = jnp.ones_like(gram[0][0])
    z, p, x = [one], [one], []
    rz = g(0, 0)
    for iteration in range(ITERS):
        q = applied(p)
        step = rz / inner(p, q)
        x = [(x[k] if k < len(x) else 0.0) + step * p[k] for k in range(len(p))]
        z = [(z[k] if k < len(z) else 0.0) - step * q[k] for k in range(len(q))]
        if iteration + 1 < ITERS:
            rz_new = inner(z, z)
            beta = rz_new / rz
            p = [z[k] + (beta * p[k] if k < len(p) else 0.0) for k in range(len(z))]
            rz = rz_new
    return x, z


def combine_kernel(members, rows, z_ref, *refs):
    basis, (scale_ref, sum_ref, x_ref, r_ref, cx, cz) = refs[:ITERS], refs[ITERS:]
    gram = [[None] * (ITERS + 1) for _ in range(ITERS + 1)]
    sums = unpacked(sum_ref[...], members)
    for n, (i, j) in enumerate(PAIRS):
        gram[i][j] = jnp.broadcast_to(sums[:, n : n + 1], (members, 128))
    x, z = coefficients(gram)
    for k in range(ITERS):
        cx[k] = x[k]
    for k in range(ITERS + 1):
        cz[k] = z[k]

    @pl.loop(0, members)
    def _(m):
        xs = [jnp.broadcast_to(cx[k, pl.ds(m, 1), :], (8, 128)) for k in range(ITERS)]
        zs = [jnp.broadcast_to(cz[k, pl.ds(m, 1), :], (8, 128)) for k in range(ITERS + 1)]
        for base in range(0, rows, 8):
            at = slice(base + HALO, base + HALO + 8)
            vs = [z_ref[m, at, :]] + [basis[k][m, at, :] for k in range(ITERS)]
            x_ref[m, base : base + 8, :] = sum((xs[k] * vs[k] for k in range(1, ITERS)), xs[0] * vs[0])
            total = sum((zs[k] * vs[k] for k in range(1, ITERS + 1)), zs[0] * vs[0])
            r_ref[m, base : base + 8, :] = scale_ref[base : base + 8, :] * total


def totals(values):
    axes = ("gx", "gy")
    counts = [lax.axis_size(axis) for axis in axes]

    def kernel(*refs):
        total_kernel(axes, counts, *refs)

    vmem = pl.BlockSpec(memory_space=pltpu.VMEM)
    return pl.pallas_call(
        kernel,
        out_shape=jax.ShapeDtypeStruct(values.shape, jnp.float32),
        in_specs=[vmem],
        out_specs=vmem,
        scratch_shapes=[pltpu.VMEM((count,) + values.shape, jnp.float32) for count in counts]
        + [pltpu.VMEM(values.shape, jnp.float32)]
        + [pltpu.SemaphoreType.DMA((count,)) for count in counts] * 2,
        compiler_params=pltpu.CompilerParams(
            collective_id=0, has_side_effects=True, vmem_limit_bytes=GRANT
        ),
    )(values)


def on_device(right_side, couplings, center, ocean_mask):
    members, rows, columns = right_side.shape
    total = rows + 2 * HALO
    planes = members + 8
    ny, nx = lax.axis_size("gy"), lax.axis_size("gx")
    vmem = pl.BlockSpec(memory_space=pltpu.VMEM)
    f32 = jnp.float32

    def halo(*refs):
        halo_kernel(members, ny, nx, *refs)

    main, strips, scale = pl.pallas_call(
        halo,
        out_shape=(
            jax.ShapeDtypeStruct((planes, total, columns), f32),
            jax.ShapeDtypeStruct((2, 3, total, columns), f32),
            jax.ShapeDtypeStruct((rows, columns), f32),
        ),
        in_specs=[vmem] * 4,
        out_specs=(vmem,) * 3,
        scratch_shapes=[
            pltpu.VMEM((3, rows, columns), f32),
            pltpu.VMEM((3, 8, columns), f32),
            pltpu.VMEM((3, 8, columns), f32),
            pltpu.VMEM((planes, 8, columns), f32),
            pltpu.VMEM((planes, 8, columns), f32),
            pltpu.VMEM((planes, 8, columns), f32),
            pltpu.VMEM((2, 3, total, columns), f32),
            pltpu.VMEM((2, 3, total, columns), f32),
            pltpu.SemaphoreType.DMA((8,)),
            pltpu.SemaphoreType.DMA((8,)),
        ],
        compiler_params=pltpu.CompilerParams(
            collective_id=1, has_side_effects=True, vmem_limit_bytes=GRANT
        ),
    )(right_side, couplings, center, ocean_mask)

    def first(*refs):
        basis_kernel(members, total, *refs)

    *basis, gram = pl.pallas_call(
        first,
        out_shape=(jax.ShapeDtypeStruct((members, total, columns), f32),) * ITERS
        + (jax.ShapeDtypeStruct((8, 128), f32),),
        in_specs=[vmem] * 3,
        out_specs=(vmem,) * (ITERS + 1),
        compiler_params=pltpu.CompilerParams(vmem_limit_bytes=GRANT),
        scratch_shapes=[pltpu.VMEM((2, 2, total, columns), f32)] * (ITERS - 1)
        + [
            pltpu.VMEM((2, 8, total, columns), f32),
            pltpu.VMEM((len(PAIRS), members, columns), f32),
        ],
    )(main, strips, scale)
    sums = totals(gram)

    def second(*refs):
        combine_kernel(members, rows, *refs)

    return pl.pallas_call(
        second,
        out_shape=(jax.ShapeDtypeStruct(right_side.shape, jnp.float32),) * 2,
        in_specs=[vmem] * (ITERS + 3),
        out_specs=(vmem, vmem),
        compiler_params=pltpu.CompilerParams(vmem_limit_bytes=GRANT),
        scratch_shapes=[
            pltpu.VMEM((ITERS, members, columns), jnp.float32),
            pltpu.VMEM((ITERS + 1, members, columns), jnp.float32),
        ],
    )(main, *basis, scale, sums)


def solution(mesh):
    in_specs = (P(None, "gy", "gx"), P(None, "gy", "gx"), P("gy", "gx"), P("gy", "gx"))
    out_specs = (P(None, "gy", "gx"), P(None, "gy", "gx"))
    return jax.shard_map(
        on_device, mesh=mesh, in_specs=in_specs, out_specs=out_specs, check_vma=False
    )
```

```python
import jax
import jax.numpy as jnp
from jax import lax
from jax.experimental import pallas as pl
from jax.experimental.pallas import tpu as pltpu
from jax.sharding import PartitionSpec as P

ITERS = 6
HALO = 8
SHIFT = 0.1
LAG = 0.05
TOGETHER = 8
GRANT = 20 * 1024 * 1024
OPPOSITE = (1, 0, 3, 2, 7, 6, 5, 4)
PAIRS = [(i, j) for i in range(ITERS) for j in range(i, ITERS + 1)]


def slots(lanes, g):
    return (lanes >= 8 * g) & (lanes < 8 * g + 8)


def reversed_tile(x, lanes, subs):
    for bit in range(7):
        step = 1 << bit
        x = jnp.where((lanes & step) == 0, pltpu.roll(x, 128 - step, 1), pltpu.roll(x, step, 1))
    for bit in range(3):
        step = 1 << bit
        x = jnp.where((subs & step) == 0, pltpu.roll(x, 8 - step, 0), pltpu.roll(x, step, 0))
    return x


def halo_kernel(
    members, ny, nx, rhs_in, coup_in, center_in, mask_in, main, strips, scale,
    rhs, coup, center, mask, load, from_west, from_south, from_corner, rows_s, rows_n, turned, packed, received, send, recv,
):
    rows = rhs.shape[1]
    tiles = rows // 8
    pairs = ((coup_in, coup), (center_in, center), (mask_in, mask), (rhs_in, rhs))
    loads = [pltpu.make_async_copy(a, b, load.at[n]) for n, (a, b) in enumerate(pairs)]
    for c in loads:
        c.start()
    planes = members + 8
    y, x = lax.axis_index("gy"), lax.axis_index("gx")
    north, south = lax.rem(y + 1, ny), lax.rem(y + ny - 1, ny)
    east, west = lax.rem(x + 1, nx), lax.rem(x + nx - 1, nx)
    mirror = nx - 1 - x
    top, bottom = y == ny - 1, y == 0
    barrier = pltpu.get_barrier_semaphore()
    peers = ((y, east), (y, west), (north, x), (south, x), (north, east), (south, west), (y, mirror))
    for there in peers:
        pl.semaphore_signal(barrier, inc=1, device_id=there, device_id_type=pl.DeviceIdType.MESH)
    pl.semaphore_wait(barrier, len(peers))

    def copy(src, dst, n, there):
        return pltpu.make_async_remote_copy(
            src_ref=src,
            dst_ref=dst,
            send_sem=send.at[n],
            recv_sem=recv.at[n],
            device_id=there,
            device_id_type=pl.DeviceIdType.MESH,
        )

    loads[0].wait()
    last_rows = coup.at[:, rows - 8 : rows, :]
    copies = [
        copy(coup, from_west, 0, (y, east)),
        copy(last_rows, from_south, 1, (north, x)),
        copy(last_rows, from_corner, 2, (north, east)),
    ]
    for c in copies:
        c.start()
    lanes = lax.broadcasted_iota(jnp.int32, (8, 128), 1)
    subs = lax.broadcasted_iota(jnp.int32, (8, 128), 0)
    first = lanes == 0
    inside = jnp.where(bottom, 0.0, 1.0)
    for c in loads[1:] + copies:
        c.wait()

    def below(ref, edge, a, t):
        if t:
            return ref[a, 8 * t - 1 : 8 * t + 7, :]
        row = jnp.broadcast_to(edge[a, 7:8, :] * inside, (8, 128))
        return jnp.where(subs == 0, row, pltpu.roll(ref[a, 0:8, :], 1, 0))

    def westward(here, beside):
        return jnp.where(first, pltpu.roll(beside, 1, 1), pltpu.roll(here, 1, 1))

    for t in range(tiles):
        at = slice(8 * t, 8 * t + 8)
        out = slice(8 * t + HALO, 8 * t + HALO + 8)
        here = [coup[a, at, :] for a in range(3)]
        prev = [below(coup, from_south, a, t) for a in range(3)]
        beside = [from_west[a, at, :] for a in range(3)]
        corner = below(from_west, from_corner, 2, t)
        terms = (
            here[0],
            prev[0],
            here[1],
            westward(here[1], beside[1]),
            here[2],
            prev[2],
            westward(here[2], beside[2]),
            westward(prev[2], corner),
        )
        diag = center[at, :] + sum(terms[1:], terms[0])
        ocean = mask[at, :].astype(jnp.float32)
        inverse = ocean / diag
        scale[at, :] = ocean * diag
        for d in range(8):
            main[members + d, out, :] = terms[d] * inverse

        @pl.loop(0, members // 8)
        def _(block):
            for within in range(8):
                m = block * 8 + within
                main[m, out, :] = rhs[m, at, :] * inverse

    up = copy(main.at[:, rows : rows + 8, :], rows_s, 3, (north, x))
    down = copy(main.at[:, 8:16, :], rows_n, 4, (south, x))
    up.start()

    @pl.when(jnp.logical_not(bottom))
    def _():
        down.start()

    @pl.when(top)
    def _():
        @pl.loop(0, members // 4)
        def _(block):
            for within in range(4):
                m = block * 4 + within
                turned[m] = reversed_tile(main[m, rows : rows + 8, :], lanes, subs)

        for d in range(8):
            tile = main[members + OPPOSITE[d], rows : rows + 8, :]
            turned[members + d] = reversed_tile(tile, lanes, subs)
        pltpu.make_async_remote_copy(
            src_ref=turned,
            dst_ref=rows_n,
            send_sem=send.at[5],
            recv_sem=recv.at[4],
            device_id=(y, mirror),
            device_id_type=pl.DeviceIdType.MESH,
        ).start()

    up.wait()
    down.wait_recv()

    @pl.when(jnp.logical_not(bottom))
    def _():
        down.wait_send()

    @pl.when(top)
    def _():
        copy(turned, rows_n, 5, (y, mirror)).wait_send()

    main[:, 0:8, :] = rows_s[...] * inside
    main[:, rows + 8 : rows + 16, :] = rows_n[...]

    @pl.loop(0, tiles + 2)
    def _(t):
        at = pl.ds(pl.multiple_of(8 * t, 8), 8)
        for group in range(3):
            eastbound = jnp.zeros((8, 128), jnp.float32)
            westbound = eastbound
            for g in range(min(16, planes - 16 * group)):
                v = main[16 * group + g, at, :]
                slot = slots(lanes, g)
                eastbound = jnp.where(slot, pltpu.roll(v, (8 * g + 8) % 128, 1), eastbound)
                westbound = jnp.where(slot, pltpu.roll(v, 8 * g, 1) if g else v, westbound)
            packed[0, group, at, :] = eastbound
            packed[1, group, at, :] = westbound

    copies = [
        copy(packed.at[0], received.at[1], 6, (y, east)),
        copy(packed.at[1], received.at[0], 7, (y, west)),
    ]
    for c in copies:
        c.start()
    for c in copies:
        c.wait()
    strips[...] = received[...]


def basis_kernel(members, rows, main_ref, strip_ref, diag_ref, *refs):
    basis, gram_ref = refs[:ITERS], refs[ITERS]
    sides, (strip_c, gram) = refs[ITERS + 1 : 2 * ITERS], refs[2 * ITERS :]
    tiles = rows // 8
    lanes = lax.broadcasted_iota(jnp.int32, (8, 128), 1)
    first, last = lanes == 0, lanes == 127
    slot_first, slot_last = lanes % 8 == 0, lanes % 8 == 7

    def field(k, m):
        return main_ref.at[m] if k == 0 else basis[k - 1].at[m]

    def side(k, s, group):
        return strip_ref.at[s, group] if k == 0 else sides[k - 1].at[s, group]

    for tile in range(tiles):
        at = slice(8 * tile, 8 * tile + 8)
        for d in range(8):
            for s in range(2):
                v = jnp.where(slots(lanes, d), strip_ref[s, 2, at, :], 0.0)
                for step in (8, 16, 32, 64):
                    v = v + pltpu.roll(v, step, 1)
                strip_c[s, d, at, :] = v

    def three(v, before, c, tile):
        base = 8 * tile
        mid = v[base : base + 8, :]
        down = v[base - 1 : base + 7, :] if tile > 0 else pltpu.roll(mid, 1, 0)
        up = v[base + 1 : base + 9, :] if tile < tiles - 1 else pltpu.roll(mid, 7, 0)
        centre = c[0] * up + c[1] * down - SHIFT * mid
        if before is not None:
            centre = centre - LAG * before[base : base + 8, :]
        return (
            centre,
            c[2] * mid + c[4] * up + c[5] * down,
            c[3] * mid + c[6] * up + c[7] * down,
        )

    for k in range(ITERS):
        final = k + 1 == ITERS
        for tile in range(1, tiles - 1) if final else range(tiles):
            at = slice(8 * tile, 8 * tile + 8)
            cm = [main_ref[members + d, at, :] for d in range(8)]
            ce = [strip_c[0, d, at, :] for d in range(8)]
            cw = [strip_c[1, d, at, :] for d in range(8)]
            for d in (2, 4, 5):
                edge = jnp.broadcast_to(cm[d][:, 127:128], (8, 128))
                ce[d] = jnp.where(slot_first, edge, pltpu.roll(ce[d], 1, 1))
                cm[d] = jnp.where(first, pltpu.roll(cw[d], 1, 1), pltpu.roll(cm[d], 1, 1))
                cw[d] = pltpu.roll(cw[d], 1, 1)
            for d in (3, 6, 7):
                edge = jnp.broadcast_to(cm[d][:, 0:1], (8, 128))
                cw[d] = jnp.where(slot_last, edge, pltpu.roll(cw[d], 127, 1))
                cm[d] = jnp.where(last, pltpu.roll(ce[d], 127, 1), pltpu.roll(cm[d], 127, 1))
                ce[d] = pltpu.roll(ce[d], 127, 1)

            @pl.loop(0, members // 16)
            def _(group):
                before = (lambda s: side(k - 1, s, group)) if k else (lambda s: None)
                mid_e, e_e, w_e = three(side(k, 0, group), before(0), ce, tile)
                mid_w, e_w, w_w = three(side(k, 1, group), before(1), cw, tile)
                into_e, into_w = pltpu.roll(w_e, 1, 1), pltpu.roll(e_w, 127, 1)
                for block in range(16 // TOGETHER):
                    outs = []
                    for g in range(block * TOGETHER, (block + 1) * TOGETHER):
                        m = group * 16 + g
                        mid, e, w = three(field(k, m), field(k - 1, m) if k else None, cm, tile)
                        shift_e = 127 - 8 * g
                        shift_w = (121 - 8 * g) % 128
                        out = mid + jnp.where(last, pltpu.roll(e_e, shift_e, 1), pltpu.roll(e, 127, 1))
                        out = out + jnp.where(first, pltpu.roll(w_w, shift_w, 1), pltpu.roll(w, 1, 1))
                        outs.append((m, out))
                        if not final:
                            into_e = jnp.where(lanes == 8 * g, pltpu.roll(w, 8 * g + 1, 1), into_e)
                            into_w = jnp.where(lanes == 8 * g + 7, pltpu.roll(e, 8 * g + 7, 1), into_w)
                    for m, out in outs:
                        basis[k][m, at, :] = out
                if not final:
                    sides[k][0, group, at, :] = mid_e + pltpu.roll(e_e, 127, 1) + into_e
                    sides[k][1, group, at, :] = mid_w + pltpu.roll(w_w, 1, 1) + into_w

    @pl.loop(0, members)
    def _(m):
        sums = [None] * len(PAIRS)
        for tile in range(tiles - 2):
            base = HALO + 8 * tile
            diag = diag_ref[8 * tile : 8 * tile + 8, :]
            vs = [field(k, m)[base : base + 8, :] for k in range(ITERS + 1)]
            scaled = [diag * v for v in vs[:ITERS]]
            for n, (i, j) in enumerate(PAIRS):
                term = scaled[i] * vs[j]
                sums[n] = term if sums[n] is None else sums[n] + term
        for n in range(len(PAIRS)):
            gram[n, pl.ds(m, 1), :] = jnp.sum(sums[n], axis=0, keepdims=True)

    wide = lax.broadcasted_iota(jnp.int32, (members, 128), 1)
    packed = jnp.zeros((members, 128), jnp.float32)
    for n in range(len(PAIRS)):
        packed = jnp.where(wide == n, jnp.sum(gram[n], axis=1, keepdims=True), packed)
    gram_ref[...] = packed_in(packed)


def packed_in(values):
    members = values.shape[0]
    groups = members // 8
    width = 128 // groups
    total = values[0:8]
    for g in range(1, groups):
        total = total + pltpu.roll(values[8 * g : 8 * g + 8], width * g, 1)
    return total


def unpacked(values, members):
    groups = members // 8
    width = 128 // groups
    parts = [values] + [pltpu.roll(values, 128 - width * g, 1) for g in range(1, groups)]
    return jnp.concatenate(parts, axis=0)


def total_kernel(axes, counts, in_ref, out_ref, *scratch):
    buffers, held = scratch[: len(axes)], scratch[len(axes)]
    send_sems, recv_sems = scratch[len(axes) + 1 : 2 * len(axes) + 1], scratch[2 * len(axes) + 1 :]
    barrier = pltpu.get_barrier_semaphore()
    for axis, count in zip(axes, counts):
        me = lax.axis_index(axis)
        for step in range(1, count):
            peer = lax.rem(me + step, count)
            pl.semaphore_signal(
                barrier, inc=1, device_id={axis: peer}, device_id_type=pl.DeviceIdType.MESH
            )
    pl.semaphore_wait(barrier, sum(counts) - len(counts))
    for stage, (axis, count) in enumerate(zip(axes, counts)):
        me = lax.axis_index(axis)
        source = in_ref if stage == 0 else held
        copies = []
        for step in range(1, count):
            peer = lax.rem(me + step, count)
            copy = pltpu.make_async_remote_copy(
                src_ref=source,
                dst_ref=buffers[stage].at[step],
                send_sem=send_sems[stage].at[step],
                recv_sem=recv_sems[stage].at[step],
                device_id={axis: peer},
                device_id_type=pl.DeviceIdType.MESH,
            )
            copy.start()
            copies.append(copy)
        for copy in copies:
            copy.wait()
        total = source[...]
        for step in range(1, count):
            total = total + buffers[stage][step]
        if stage + 1 < len(axes):
            held[...] = total
        else:
            out_ref[...] = total


def coefficients(gram):
    def g(i, j):
        return gram[min(i, j)][max(i, j)]

    def applied(p):
        q = []
        for k in range(ITERS + 1):
            terms = []
            if k < len(p):
                terms.append((1.0 - SHIFT) * p[k])
            if 0 < k <= len(p):
                terms.append(-p[k - 1])
            if k + 1 < len(p):
                terms.append(-LAG * p[k + 1])
            if terms:
                q.append(sum(terms[1:], terms[0]))
        return q

    def inner(p, q):
        total = None
        for i, a in enumerate(p):
            row = None
            for j, b in enumerate(q):
                t = g(i, j) * b
                row = t if row is None else row + t
            t = a * row
            total = t if total is None else total + t
        return total

    one = jnp.ones_like(gram[0][0])
    z, p, x = [one], [one], []
    rz = g(0, 0)
    for iteration in range(ITERS):
        q = applied(p)
        step = rz / inner(p, q)
        x = [(x[k] if k < len(x) else 0.0) + step * p[k] for k in range(len(p))]
        z = [(z[k] if k < len(z) else 0.0) - step * q[k] for k in range(len(q))]
        if iteration + 1 < ITERS:
            rz_new = inner(z, z)
            beta = rz_new / rz
            p = [z[k] + (beta * p[k] if k < len(p) else 0.0) for k in range(len(z))]
            rz = rz_new
    return x, z


def combine_kernel(members, rows, z_ref, *refs):
    basis, (scale_ref, sum_ref, x_ref, r_ref, cx, cz) = refs[:ITERS], refs[ITERS:]
    gram = [[None] * (ITERS + 1) for _ in range(ITERS + 1)]
    sums = unpacked(sum_ref[...], members)
    for n, (i, j) in enumerate(PAIRS):
        gram[i][j] = jnp.broadcast_to(sums[:, n : n + 1], (members, 128))
    x, z = coefficients(gram)
    for k in range(ITERS):
        cx[k] = x[k]
    for k in range(ITERS + 1):
        cz[k] = z[k]

    @pl.loop(0, members)
    def _(m):
        xs = [jnp.broadcast_to(cx[k, pl.ds(m, 1), :], (8, 128)) for k in range(ITERS)]
        zs = [jnp.broadcast_to(cz[k, pl.ds(m, 1), :], (8, 128)) for k in range(ITERS + 1)]
        for base in range(0, rows, 8):
            at = slice(base + HALO, base + HALO + 8)
            vs = [z_ref[m, at, :]] + [basis[k][m, at, :] for k in range(ITERS)]
            x_ref[m, base : base + 8, :] = sum((xs[k] * vs[k] for k in range(1, ITERS)), xs[0] * vs[0])
            total = sum((zs[k] * vs[k] for k in range(1, ITERS + 1)), zs[0] * vs[0])
            r_ref[m, base : base + 8, :] = scale_ref[base : base + 8, :] * total


def totals(values):
    axes = ("gx", "gy")
    counts = [lax.axis_size(axis) for axis in axes]

    def kernel(*refs):
        total_kernel(axes, counts, *refs)

    vmem = pl.BlockSpec(memory_space=pltpu.VMEM)
    return pl.pallas_call(
        kernel,
        out_shape=jax.ShapeDtypeStruct(values.shape, jnp.float32),
        in_specs=[vmem],
        out_specs=vmem,
        scratch_shapes=[pltpu.VMEM((count,) + values.shape, jnp.float32) for count in counts]
        + [pltpu.VMEM(values.shape, jnp.float32)]
        + [pltpu.SemaphoreType.DMA((count,)) for count in counts] * 2,
        compiler_params=pltpu.CompilerParams(
            collective_id=0, has_side_effects=True, vmem_limit_bytes=GRANT
        ),
    )(values)


def on_device(right_side, couplings, center, ocean_mask):
    members, rows, columns = right_side.shape
    total = rows + 2 * HALO
    planes = members + 8
    ny, nx = lax.axis_size("gy"), lax.axis_size("gx")
    vmem = pl.BlockSpec(memory_space=pltpu.VMEM)
    f32 = jnp.float32

    def halo(*refs):
        halo_kernel(members, ny, nx, *refs)

    main, strips, scale = pl.pallas_call(
        halo,
        out_shape=(
            jax.ShapeDtypeStruct((planes, total, columns), f32),
            jax.ShapeDtypeStruct((2, 3, total, columns), f32),
            jax.ShapeDtypeStruct((rows, columns), f32),
        ),
        in_specs=[pl.BlockSpec(memory_space=pltpu.HBM)] * 4,
        out_specs=(vmem,) * 3,
        scratch_shapes=[
            pltpu.VMEM(right_side.shape, f32),
            pltpu.VMEM(couplings.shape, f32),
            pltpu.VMEM(center.shape, f32),
            pltpu.VMEM(ocean_mask.shape, ocean_mask.dtype),
            pltpu.SemaphoreType.DMA((4,)),
            pltpu.VMEM((3, rows, columns), f32),
            pltpu.VMEM((3, 8, columns), f32),
            pltpu.VMEM((3, 8, columns), f32),
            pltpu.VMEM((planes, 8, columns), f32),
            pltpu.VMEM((planes, 8, columns), f32),
            pltpu.VMEM((planes, 8, columns), f32),
            pltpu.VMEM((2, 3, total, columns), f32),
            pltpu.VMEM((2, 3, total, columns), f32),
            pltpu.SemaphoreType.DMA((8,)),
            pltpu.SemaphoreType.DMA((8,)),
        ],
        compiler_params=pltpu.CompilerParams(
            collective_id=1, has_side_effects=True, vmem_limit_bytes=GRANT
        ),
    )(right_side, couplings, center, ocean_mask)

    def first(*refs):
        basis_kernel(members, total, *refs)

    *basis, gram = pl.pallas_call(
        first,
        out_shape=(jax.ShapeDtypeStruct((members, total, columns), f32),) * ITERS
        + (jax.ShapeDtypeStruct((8, 128), f32),),
        in_specs=[vmem] * 3,
        out_specs=(vmem,) * (ITERS + 1),
        compiler_params=pltpu.CompilerParams(vmem_limit_bytes=GRANT),
        scratch_shapes=[pltpu.VMEM((2, 2, total, columns), f32)] * (ITERS - 1)
        + [
            pltpu.VMEM((2, 8, total, columns), f32),
            pltpu.VMEM((len(PAIRS), members, columns), f32),
        ],
    )(main, strips, scale)
    sums = totals(gram)

    def second(*refs):
        combine_kernel(members, rows, *refs)

    return pl.pallas_call(
        second,
        out_shape=(jax.ShapeDtypeStruct(right_side.shape, jnp.float32),) * 2,
        in_specs=[vmem] * (ITERS + 3),
        out_specs=(vmem, vmem),
        compiler_params=pltpu.CompilerParams(vmem_limit_bytes=GRANT),
        scratch_shapes=[
            pltpu.VMEM((ITERS, members, columns), jnp.float32),
            pltpu.VMEM((ITERS + 1, members, columns), jnp.float32),
        ],
    )(main, *basis, scale, sums)


def solution(mesh):
    in_specs = (P(None, "gy", "gx"), P(None, "gy", "gx"), P("gy", "gx"), P("gy", "gx"))
    out_specs = (P(None, "gy", "gx"), P(None, "gy", "gx"))
    return jax.shard_map(
        on_device, mesh=mesh, in_specs=in_specs, out_specs=out_specs, check_vma=False
    )
```
